32 devices in a mesh: ba: 4 (over x, core), gx: 2 (over y), gy: 4 (over z).
Axes of the slice: x: 2, y: 2, z: 4, core: 2. Of those that a mesh axis runs over, the one named last changes fastest.
Arguments:
- pixels: bfloat16 [112, 224, 6], P(('ba', 'gx'), 'gy'), parts along dimension 0, may hold values from -6 to 6
- conv_weight: bfloat16 [54, 704], replicated, may hold values from -0.875 to 0.875
- input_gain: float32 [704], replicated, may hold values from 0.5 to 1.5
- key_weight: bfloat16 [704, 1024], replicated, may hold values from -0.21875 to 0.21875
- value_weight: bfloat16 [704, 1024], replicated, may hold values from -0.21875 to 0.21875
- latents: bfloat16 [512, 1024], replicated, may hold values from -6 to 6
- latent_gain: float32 [1024], replicated, may hold values from 0.5 to 1.5
- query_weight: bfloat16 [1024, 1024], replicated, as said below
- out_weight: bfloat16 [1024, 1024], replicated, may hold values from -0.1875 to 0.1875
Outputs:
- new_latents: bfloat16 [2048, 1024], P(('ba', 'gx', 'gy')), parts along dimension 0
The draws below stay inside these ranges and needn't reach their ends.
There are 4 independent parts, one for each index of `ba`. The reference program is written for one: setup_inputs(seed, part) draws one part's arguments, and reference() takes and returns one part's arrays. A program takes and returns all parts, laid end to end along the dimension named above; an argument that names none is the same for every part. Nothing has to cross between parts.
Inputs may be any that keep to these rules, and one draw needn't show every extreme that they name: `query_weight`: independent entries, mean zero, of order 3 * 1024 ** -0.5, and up to 20 times that in the columns of some heads.
All inputs are finite; a program needn't handle non-finite values.
Results may differ from the reference program's by a relative error of at most 0.025.
Values may be sent and summed in bfloat16 or wider, within the bound.
A program may use at most 64 MiB of HBM per device.

```python
import math
import jax
import jax.numpy as jnp
from jax import lax

C_IN = 6
FEAT = 704
D = 1024
HEADS = 8
LAT = 512
DH = 128
H = 28
W = 224


def draw_query_weight(key, part):
    base = jax.random.truncated_normal(key, -5.0, 5.0, (D, D), jnp.float32) * (3.0 / math.sqrt(D))
    strong = jax.random.randint(jax.random.fold_in(key, 11), (), 0, HEADS)
    head_scale = jnp.where(jnp.arange(HEADS) == strong, 16.0, 1.0).astype(jnp.float32)
    base = base * jnp.repeat(head_scale, D // HEADS)[None, :]
    return base.astype(jnp.bfloat16)


def block_scale(stream_key, dims, pieces, smallest, largest):
    def one(position, blocks):
        steps = jax.random.uniform(jax.random.fold_in(jax.random.fold_in(stream_key, 6), position), (blocks,), jnp.float32, smallest / len(pieces), largest / len(pieces))
        return jnp.repeat(jnp.exp(steps), dims[position] // blocks).reshape((-1,) + (1,) * (len(dims) - position - 1))

    level = one(*pieces[0])
    for cut in pieces[1:]:
        level = level * one(*cut)
    return level


def gaussian(stream_key, extent, scale, reach, cuts=(), kind=jnp.bfloat16):
    values = jax.random.normal(stream_key, extent, jnp.float32) * scale
    if len(cuts) > 0:
        values = block_scale(stream_key, extent, cuts, -0.22, 0.18) * values
    return jnp.clip(values, min=-reach, max=reach).astype(kind)


def setup_inputs(seed: int = 0, part: int = 0) -> dict:
    seeds = jax.random.split(jax.random.key(seed), 10)
    part_keys = jax.random.split(jax.random.fold_in(seeds[9], part), 10)
    return {
        "pixels": gaussian(part_keys[0], (H, W, C_IN), 1.0, 6.0, ((0, 2), (1, 4))),
        "conv_weight": gaussian(seeds[1], (9 * C_IN, FEAT), (9 * C_IN) ** -0.5, 0.875),
        "input_gain": jnp.clip(1.0 + 0.1 * jax.random.normal(seeds[2], (FEAT,), jnp.float32), 0.5, 1.5),
        "key_weight": gaussian(seeds[3], (FEAT, D), FEAT ** -0.5, 0.21875),
        "value_weight": gaussian(seeds[4], (FEAT, D), FEAT ** -0.5, 0.21875),
        "latents": gaussian(seeds[5], (LAT, D), 1.0, 6.0),
        "latent_gain": jnp.clip(1.0 + 0.1 * jax.random.normal(seeds[6], (D,), jnp.float32), 0.5, 1.5),
        "query_weight": draw_query_weight(jax.random.fold_in(seeds[9], 71), part),
        "out_weight": gaussian(seeds[8], (D, D), D ** -0.5, 0.1875),
    }


def layer_norm(values, gain):
    mean = lax.optimization_barrier(jnp.mean(values, axis=-1, keepdims=True))
    centred = values - mean
    variance = lax.optimization_barrier(jnp.mean(centred * centred, axis=-1, keepdims=True))
    return centred * lax.rsqrt(variance + 1e-05) * gain

def reference(pixels, conv_weight, input_gain, key_weight, value_weight, latents, latent_gain, query_weight, out_weight):
    height, width = (pixels.shape[0], pixels.shape[1])
    padded = jnp.pad(pixels, ((1, 1), (1, 1), (0, 0)))
    patches = jnp.concatenate([padded[row_off:row_off + height, col_off:col_off + width, :] for row_off in range(3) for col_off in range(3)], axis=-1)
    patches = patches.reshape(height * width, -1)
    features = jnp.dot(patches, conv_weight, preferred_element_type=jnp.float32).astype(jnp.bfloat16)
    normed = layer_norm(features.astype(jnp.float32), input_gain.astype(jnp.float32)).astype(jnp.bfloat16)
    key_rows = jnp.dot(normed, key_weight, preferred_element_type=jnp.float32).astype(jnp.bfloat16)
    value_rows = jnp.dot(normed, value_weight, preferred_element_type=jnp.float32).astype(jnp.bfloat16)
    lat_normed = layer_norm(latents.astype(jnp.float32), latent_gain.astype(jnp.float32)).astype(jnp.bfloat16)
    queries = jnp.dot(lat_normed, query_weight, preferred_element_type=jnp.float32).astype(jnp.bfloat16)
    scale = 1.0 / DH ** 0.5

    def one_head(head):
        start = (head * DH).astype(jnp.int32)
        query_head = lax.dynamic_slice_in_dim(queries, start, DH, 1)
        key_head = lax.dynamic_slice_in_dim(key_rows, start, DH, 1)
        value_head = lax.dynamic_slice_in_dim(value_rows, start, DH, 1)
        scores = jnp.dot(query_head, key_head.T, preferred_element_type=jnp.float32) * scale
        expo = jnp.exp(scores - lax.optimization_barrier(jnp.max(scores, axis=-1, keepdims=True)))
        total = lax.optimization_barrier(jnp.sum(expo, axis=-1))
        summed = jnp.dot(expo.astype(jnp.bfloat16), value_head, preferred_element_type=jnp.float32)
        return summed / total[:, None]
    per_head = lax.map(one_head, jnp.arange(HEADS, dtype=jnp.int32))
    attended = jnp.transpose(per_head, (1, 0, 2)).reshape(LAT, D).astype(jnp.bfloat16)
    result = latents.astype(jnp.float32) + jnp.dot(attended, out_weight, preferred_element_type=jnp.float32)
    return result.astype(jnp.bfloat16)
```

```python
import functools
import math

import jax
import jax.numpy as jnp
from jax import lax
from jax.experimental import pallas as pl
from jax.experimental.pallas import tpu as pltpu
from jax.sharding import PartitionSpec as P

DH = 128
MESH = pl.DeviceIdType.MESH
BF = jnp.bfloat16
F32 = jnp.float32


def mm(a, b, precision=None):
    return lax.dot_general(
        a, b, (((1,), (0,)), ((), ())), precision=precision, preferred_element_type=F32
    )


def mm_nt(a, b):
    return lax.dot_general(a, b, (((1,), (1,)), ((), ())), preferred_element_type=F32)


def split(x):
    hi = x.astype(BF).astype(F32)
    return hi, x - hi


def kernel(
    dims,
    px_ref,
    conv_ref,
    gain_ref,
    lgain_ref,
    wk_ref,
    wv_ref,
    lat_ref,
    wq_ref,
    wo_ref,
    out_ref,
    tiles,
    stack,
    conv8,
    wk,
    wv,
    wq,
    lat,
    own,
    wo,
    acc,
    top,
    att_src,
    att,
    copy_sem,
    send1,
    recv1,
    send2,
    recv2,
):
    ngx, ngy, tr, tc, heads, taps, chans = dims
    g = ngx * ngy
    blocks = g // heads
    share = own.shape[0]
    rows = lat.shape[0]
    width = px_ref.shape[1]
    cells = tr * tc
    ch = px_ref.shape[0]
    pk = taps * ch
    me = lax.axis_index("gx") * ngy + lax.axis_index("gy")
    head = lax.rem(me, heads)
    block = me // heads

    col = pl.ds(pl.multiple_of(head * DH, DH), DH)
    lat_rows = pl.ds(pl.multiple_of(block * rows, rows), rows)
    own_rows = pl.ds(pl.multiple_of(me * share, share), share)
    loads = [
        pltpu.make_async_copy(px_ref, tiles.at[me], copy_sem.at[0]),
        pltpu.make_async_copy(lat_ref.at[lat_rows, :], lat, copy_sem.at[1]),
        pltpu.make_async_copy(wq_ref.at[:, col], wq, copy_sem.at[2]),
        pltpu.make_async_copy(wk_ref.at[:, col], wk, copy_sem.at[3]),
        pltpu.make_async_copy(wv_ref.at[:, col], wv, copy_sem.at[4]),
        pltpu.make_async_copy(lat_ref.at[own_rows, :], own, copy_sem.at[5]),
        pltpu.make_async_copy(wo_ref, wo, copy_sem.at[6]),
    ]
    for load in loads:
        load.start()

    def place(p):
        return {"gx": p // ngy, "gy": lax.rem(p, ngy)}

    barrier = pltpu.get_barrier_semaphore()
    for k in range(1, g):
        pl.semaphore_signal(
            barrier, inc=1, device_id=place(lax.rem(me + k, g)), device_id_type=MESH
        )
    pl.semaphore_wait(barrier, g - 1)
    sends = []
    for k in range(1, g):
        send = pltpu.make_async_remote_copy(
            src_ref=px_ref,
            dst_ref=tiles.at[me],
            send_sem=send1.at[k],
            recv_sem=recv1.at[k],
            device_id=place(lax.rem(me + k, g)),
            device_id_type=MESH,
        )
        send.start()
        sends.append(send)

    conv8[...] = jnp.zeros_like(conv8)
    for s in range(taps):
        conv8[s * ch : s * ch + chans, :] = conv_ref[s * chans : (s + 1) * chans, :].astype(F32)
    conv = conv8[...]
    centred = conv - jnp.mean(conv, axis=-1, keepdims=True)
    gained_hi, gained_lo = split(centred * gain_ref[...])
    gained = jnp.concatenate([gained_hi, gained_lo], axis=0).astype(BF)
    doubled = jnp.transpose(jnp.concatenate([centred, centred], axis=0))
    lane2 = lax.broadcasted_iota(jnp.int32, doubled.shape, 1)
    d_hi, d_lo = split(doubled)
    conv_t = jnp.where(lane2 < pk, d_hi, d_lo).astype(BF)

    loads[1].wait()
    loads[2].wait()
    rows_f = lat[...].astype(F32)
    mean = jnp.mean(rows_f, axis=-1, keepdims=True)
    rows_c = rows_f - mean
    var = jnp.mean(rows_c * rows_c, axis=-1, keepdims=True)
    lat_normed = (rows_c * lax.rsqrt(var + 1e-05) * lgain_ref[...]).astype(BF)
    query = mm(lat_normed, wq[...]).astype(BF)
    loads[3].wait()
    loads[4].wait()
    mk2 = mm(gained, wk[...])
    mv2 = mm(gained, wv[...])
    mk = mk2[:pk] + mk2[pk:]
    mv = mv2[:pk] + mv2[pk:]
    mk_hi, mk_lo = split(mk)
    mk3_hi = jnp.concatenate([mk_hi] * 3, axis=0).astype(BF)
    mk3_lo = jnp.concatenate([mk_lo] * 3, axis=0).astype(BF)
    q3 = (mm_nt(query, mk3_hi) + mm_nt(query, mk3_lo)) * (math.log2(math.e) / DH**0.5)
    q_hi, q_lo = split(q3)
    lane3 = lax.broadcasted_iota(jnp.int32, q3.shape, 1)
    q3 = jnp.where((lane3 >= pk) & (lane3 < 2 * pk), q_lo, q_hi)
    q3 = jnp.where(lane3 == chans, 1.0, q3).astype(BF)

    loads[0].wait()
    for k, send in enumerate(sends, 1):
        came = pltpu.make_async_remote_copy(
            src_ref=px_ref,
            dst_ref=tiles.at[lax.rem(me + g - k, g)],
            send_sem=send1.at[k],
            recv_sem=recv1.at[k],
            device_id=place(lax.rem(me + g - k, g)),
            device_id_type=MESH,
        )
        came.wait_recv()

    lane = lax.broadcasted_iota(jnp.int32, (ch, width), 1)
    tile_row = lane // tc
    tile_col = lane - tile_row * tc
    low_row, high_row = tile_row == 0, tile_row == tr - 1
    low_col, high_col = tile_col == 0, tile_col == tc - 1

    def roll(x, shift):
        return pltpu.roll(x, shift % width, 1)

    def build(t):
        static = isinstance(t, int)
        i = t // ngy
        j = t - i * ngy

        def get(di, dj):
            if static:
                if 0 <= i + di < ngx and 0 <= j + dj < ngy:
                    return tiles[t + di * ngy + dj]
                return None
            inside = (i + di >= 0) & (i + di < ngx) & (j + dj >= 0) & (j + dj < ngy)
            at = jnp.clip(t + di * ngy + dj, 0, g - 1)
            return tiles[at] * jnp.where(inside, 1.0, 0.0)

        def pick(mask, edge, edge_shift, inner, inner_shift):
            if inner is None and edge is None:
                return None
            a = jnp.zeros((ch, width), F32) if edge is None else roll(edge, edge_shift)
            b = jnp.zeros((ch, width), F32) if inner is None else roll(inner, inner_shift)
            return jnp.where(mask, a, b)

        def columns(di):
            mid = get(di, 0)
            left = pick(low_col, get(di, -1), 1 - tc, mid, 1)
            right = pick(high_col, get(di, 1), tc - 1, mid, -1)
            return left, mid, right

        above, here, below = columns(-1), columns(0), columns(1)
        reach = (tr - 1) * tc
        parts = [pick(low_row, a, -reach, h, tc) for a, h in zip(above, here)]
        parts += list(here)
        parts += [pick(high_row, b, reach, h, -tc) for b, h in zip(below, here)]
        patches = jnp.concatenate(parts, axis=0)
        twice = jnp.concatenate([patches, patches], axis=0).astype(BF)
        feats = mm(conv_t, twice)
        variance = jnp.sum(feats * feats, axis=0, keepdims=True) * (1.0 / conv_t.shape[0])
        scaled = patches * lax.rsqrt(variance + 1e-05)
        hi, lo = split(scaled)
        full = jnp.concatenate([hi, hi, lo], axis=0)
        row3 = lax.broadcasted_iota(jnp.int32, full.shape, 0)
        cell3 = lax.broadcasted_iota(jnp.int32, full.shape, 1)
        full = jnp.where((row3 == chans) & (cell3 >= cells), -1e30, full)
        full = jnp.where(row3 == chans + 1, 1.0, full)
        stack[t] = full.astype(BF)

    def attend(t, first):
        block_px = stack[t]
        scores = mm(q3, block_px)
        high = jnp.max(scores, axis=-1, keepdims=True)
        if not first:
            high = jnp.maximum(high, top[...])
        expo = jnp.exp2(scores - high).astype(BF)
        part = mm_nt(expo, block_px)
        if first:
            acc[...] = part
        else:
            acc[...] = acc[...] * jnp.exp2(top[...] - high) + part
        top[...] = high

    if g <= 8:
        for t in range(g):
            build(t)
        for t in range(g):
            attend(t, t == 0)
    else:
        pl.loop(0, g)(build)
        attend(0, True)
        pl.loop(1, g)(lambda t: attend(t, False))

    summed = acc[...]
    lane_s = lax.broadcasted_iota(jnp.int32, summed.shape, 1)
    total = jnp.sum(jnp.where(lane_s == chans + 1, summed, 0.0), axis=-1, keepdims=True)
    mv3 = jnp.concatenate([mv, jnp.zeros_like(mv), mv], axis=0)
    attended = mm(summed / total, mv3, precision=lax.Precision.HIGHEST)
    att_src[...] = attended.astype(BF).reshape(heads, share, DH)

    mine = pltpu.make_async_copy(att_src.at[head], att.at[head], copy_sem.at[7])
    mine.start()
    sends2 = []
    for k in range(1, heads):
        to = lax.rem(head + k, heads)
        send = pltpu.make_async_remote_copy(
            src_ref=att_src.at[to],
            dst_ref=att.at[head],
            send_sem=send2.at[k],
            recv_sem=recv2.at[k],
            device_id=place(block * heads + to),
            device_id_type=MESH,
        )
        send.start()
        sends2.append(send)
    for send in sends:
        send.wait_send()
    loads[5].wait()
    loads[6].wait()
    mine.wait()
    for k in range(1, heads):
        source = lax.rem(head + heads - k, heads)
        came = pltpu.make_async_remote_copy(
            src_ref=att_src.at[source],
            dst_ref=att.at[source],
            send_sem=send2.at[k],
            recv_sem=recv2.at[k],
            device_id=place(block * heads + source),
            device_id_type=MESH,
        )
        came.wait_recv()
    gathered = jnp.concatenate([att[h] for h in range(heads)], axis=1)
    out_ref[...] = (own[...].astype(F32) + mm(gathered, wo[...])).astype(BF)
    for send in sends2:
        send.wait_send()


def on_device(
    pixels,
    conv_weight,
    input_gain,
    key_weight,
    value_weight,
    latents,
    latent_gain,
    query_weight,
    out_weight,
):
    tr, tc, chans = pixels.shape
    ngx, ngy = lax.axis_size("gx"), lax.axis_size("gy")
    g = ngx * ngy
    lat_count, width_d = latents.shape
    heads = width_d // DH
    share = lat_count // g
    rows = share * heads
    feat = conv_weight.shape[1]
    taps = conv_weight.shape[0] // chans
    width = -(-tr * tc // 128) * 128
    ch = -(-(chans + 2) // 8) * 8
    flat = jnp.transpose(pixels, (2, 0, 1)).reshape(chans, tr * tc).astype(F32)
    flat = jnp.pad(flat, ((0, ch - chans), (0, width - tr * tc)))
    pk = taps * ch
    vmem = pl.BlockSpec(memory_space=pltpu.VMEM)
    hbm = pl.BlockSpec(memory_space=pl.ANY)
    return pl.pallas_call(
        functools.partial(kernel, (ngx, ngy, tr, tc, heads, taps, chans)),
        out_shape=jax.ShapeDtypeStruct((share, width_d), BF),
        in_specs=[vmem] * 4 + [hbm] * 5,
        out_specs=vmem,
        scratch_shapes=[
            pltpu.VMEM((g, ch, width), F32),
            pltpu.VMEM((g, 3 * pk, width), BF),
            pltpu.VMEM((pk, feat), F32),
            pltpu.VMEM((feat, DH), BF),
            pltpu.VMEM((feat, DH), BF),
            pltpu.VMEM((width_d, DH), BF),
            pltpu.VMEM((rows, width_d), BF),
            pltpu.VMEM((share, width_d), BF),
            pltpu.VMEM((width_d, width_d), BF),
            pltpu.VMEM((rows, 3 * pk), F32),
            pltpu.VMEM((rows, 1), F32),
            pltpu.VMEM((heads, share, DH), BF),
            pltpu.VMEM((heads, share, DH), BF),
            pltpu.SemaphoreType.DMA((8,)),
            pltpu.SemaphoreType.DMA((g,)),
            pltpu.SemaphoreType.DMA((g,)),
            pltpu.SemaphoreType.DMA((heads,)),
            pltpu.SemaphoreType.DMA((heads,)),
        ],
        compiler_params=pltpu.CompilerParams(
            collective_id=0, has_side_effects=True, vmem_limit_bytes=56 * 1024 * 1024
        ),
    )(
        flat,
        conv_weight,
        input_gain.reshape(1, -1),
        latent_gain.reshape(1, -1),
        key_weight,
        value_weight,
        latents,
        query_weight,
        out_weight,
    )


def solution(mesh):
    return jax.shard_map(
        on_device,
        mesh=mesh,
        in_specs=(P(("ba", "gx"), "gy", None), P(), P(), P(), P(), P(), P(), P(), P()),
        out_specs=P(("ba", "gx", "gy"), None),
        check_vma=False,
    )
```

```python
import functools
import math

import jax
import jax.numpy as jnp
from jax import lax
from jax.experimental import pallas as pl
from jax.experimental.pallas import tpu as pltpu
from jax.sharding import PartitionSpec as P

DH = 128
MESH = pl.DeviceIdType.MESH
BF = jnp.bfloat16
F32 = jnp.float32


def mm(a, b, precision=None):
    return lax.dot_general(
        a, b, (((1,), (0,)), ((), ())), precision=precision, preferred_element_type=F32
    )


def mm_nt(a, b):
    return lax.dot_general(a, b, (((1,), (1,)), ((), ())), preferred_element_type=F32)


def split(x):
    hi = x.astype(BF).astype(F32)
    return hi, x - hi


def kernel(
    dims,
    px_hbm,
    conv_hbm,
    gain_hbm,
    lgain_hbm,
    wk_ref,
    wv_ref,
    lat_ref,
    wq_ref,
    wo_ref,
    out_ref,
    px_raw,
    px_wide,
    px_ref,
    conv_ref,
    gain_ref,
    lgain_ref,
    code_ref,
    patch_ref,
    tiles,
    stack,
    conv8,
    wk,
    wv,
    wq,
    lat,
    own,
    wo,
    acc,
    top,
    att_src,
    att,
    copy_sem,
    send1,
    recv1,
    send2,
    recv2,
):
    ngx, ngy, tr, tc, heads, taps, chans = dims
    g = ngx * ngy
    blocks = g // heads
    share = own.shape[0]
    rows = lat.shape[0]
    width = px_ref.shape[1]
    compact = g <= 8
    cells = tr * tc
    ch = px_ref.shape[0]
    pk = taps * ch
    me = lax.axis_index("gx") * ngy + lax.axis_index("gy")
    head = lax.rem(me, heads)
    block = me // heads

    col = pl.ds(pl.multiple_of(head * DH, DH), DH)
    lat_rows = pl.ds(pl.multiple_of(block * rows, rows), rows)
    own_rows = pl.ds(pl.multiple_of(me * share, share), share)
    def place(p):
        return {"gx": p // ngy, "gy": lax.rem(p, ngy)}

    barrier = pltpu.get_barrier_semaphore()
    for k in range(1, g):
        pl.semaphore_signal(
            barrier, inc=1, device_id=place(lax.rem(me + k, g)), device_id_type=MESH
        )
    early = [
        pltpu.make_async_copy(px_hbm, px_raw, copy_sem.at[8]),
        pltpu.make_async_copy(conv_hbm, conv_ref, copy_sem.at[9]),
        pltpu.make_async_copy(gain_hbm, gain_ref, copy_sem.at[10]),
        pltpu.make_async_copy(lgain_hbm, lgain_ref, copy_sem.at[11]),
    ]
    for load in early:
        load.start()
    own_tile = pltpu.make_async_copy(px_ref, tiles.at[me], copy_sem.at[0])
    loads = [
        own_tile,
        pltpu.make_async_copy(lat_ref.at[lat_rows, :], lat, copy_sem.at[1]),
        pltpu.make_async_copy(wq_ref.at[:, col], wq, copy_sem.at[2]),
        pltpu.make_async_copy(wk_ref.at[:, col], wk, copy_sem.at[3]),
        pltpu.make_async_copy(wv_ref.at[:, col], wv, copy_sem.at[4]),
        pltpu.make_async_copy(lat_ref.at[own_rows, :], own, copy_sem.at[5]),
        pltpu.make_async_copy(wo_ref, wo, copy_sem.at[6]),
    ]
    for load in loads[1:]:
        load.start()

    px_wide[...] = jnp.zeros_like(px_wide)
    if compact:
        spot = lax.broadcasted_iota(jnp.int32, (ch, g * cells), 1)
        tile = spot // cells
        inner = spot - tile * cells
        r = inner // tc
        c = inner - r * tc
        ti = tile // ngy
        tj = tile - ti * ngy
        code = jnp.zeros_like(spot)
        tests = (
            c == 0, c == tc - 1, r == 0, r == tr - 1,
            tj == 0, tj == ngy - 1, ti == 0, ti == ngx - 1,
        )
        for bit, test in enumerate(tests):
            code = code + jnp.where(test, 1 << bit, 0)
        code_ref[...] = code
    early[0].wait()
    raw = px_raw[...].astype(F32)
    px_wide[0:chans, 0:cells] = jnp.concatenate([raw[:, r, :] for r in range(tr)], axis=1)
    px_ref[...] = px_wide[...].astype(BF)
    own_tile.start()
    pl.semaphore_wait(barrier, g - 1)
    sends = []
    for k in range(1, g):
        send = pltpu.make_async_remote_copy(
            src_ref=px_ref,
            dst_ref=tiles.at[me],
            send_sem=send1.at[k],
            recv_sem=recv1.at[k],
            device_id=place(lax.rem(me + k, g)),
            device_id_type=MESH,
        )
        send.start()
        sends.append(send)

    for load in early[1:]:
        load.wait()
    conv8[...] = jnp.zeros_like(conv8)
    for s in range(taps):
        conv8[s * ch : s * ch + chans, :] = conv_ref[s * chans : (s + 1) * chans, :].astype(F32)
    conv = conv8[...]
    centred = conv - jnp.mean(conv, axis=-1, keepdims=True)
    gained_hi, gained_lo = split(centred * gain_ref[...].reshape(1, -1))
    gained = jnp.concatenate([gained_hi, gained_lo], axis=0).astype(BF)
    doubled = jnp.transpose(jnp.concatenate([centred, centred], axis=0))
    lane2 = lax.broadcasted_iota(jnp.int32, doubled.shape, 1)
    d_hi, d_lo = split(doubled)
    conv_t = jnp.where(lane2 < pk, d_hi, d_lo).astype(BF)

    loads[1].wait()
    loads[2].wait()
    rows_f = lat[...].astype(F32)
    mean = jnp.mean(rows_f, axis=-1, keepdims=True)
    rows_c = rows_f - mean
    var = jnp.mean(rows_c * rows_c, axis=-1, keepdims=True)
    lat_normed = (rows_c * lax.rsqrt(var + 1e-05) * lgain_ref[...].reshape(1, -1)).astype(BF)
    query = mm(lat_normed, wq[...]).astype(BF)
    loads[3].wait()
    loads[4].wait()
    mk2 = mm(gained, wk[...])
    mv2 = mm(gained, wv[...])
    mk = mk2[:pk] + mk2[pk:]
    mv = mv2[:pk] + mv2[pk:]
    mk_hi, mk_lo = split(mk)
    mk3_hi = jnp.concatenate([mk_hi] * 3, axis=0).astype(BF)
    mk3_lo = jnp.concatenate([mk_lo] * 3, axis=0).astype(BF)
    q3 = (mm_nt(query, mk3_hi) + mm_nt(query, mk3_lo)) * (math.log2(math.e) / DH**0.5)
    q_hi, q_lo = split(q3)
    lane3 = lax.broadcasted_iota(jnp.int32, q3.shape, 1)
    q3 = jnp.where((lane3 >= pk) & (lane3 < 2 * pk), q_lo, q_hi)
    q3 = jnp.where(lane3 == chans, 1.0, q3).astype(BF)

    loads[0].wait()
    for k, send in enumerate(sends, 1):
        came = pltpu.make_async_remote_copy(
            src_ref=px_ref,
            dst_ref=tiles.at[lax.rem(me + g - k, g)],
            send_sem=send1.at[k],
            recv_sem=recv1.at[k],
            device_id=place(lax.rem(me + g - k, g)),
            device_id_type=MESH,
        )
        came.wait_recv()

    lane = lax.broadcasted_iota(jnp.int32, (ch, width), 1)
    tile_row = lane // tc
    tile_col = lane - tile_row * tc
    low_row, high_row = tile_row == 0, tile_row == tr - 1
    low_col, high_col = tile_col == 0, tile_col == tc - 1

    def roll(x, shift):
        return pltpu.roll(x, shift % width, 1)

    def build(t):
        static = isinstance(t, int)
        i = t // ngy
        j = t - i * ngy

        def get(di, dj):
            if static:
                if 0 <= i + di < ngx and 0 <= j + dj < ngy:
                    return tiles[t + di * ngy + dj].astype(F32)
                return None
            inside = (i + di >= 0) & (i + di < ngx) & (j + dj >= 0) & (j + dj < ngy)
            at = jnp.clip(t + di * ngy + dj, 0, g - 1)
            return tiles[at].astype(F32) * jnp.where(inside, 1.0, 0.0)

        def pick(mask, edge, edge_shift, inner, inner_shift):
            if inner is None and edge is None:
                return None
            a = jnp.zeros((ch, width), F32) if edge is None else roll(edge, edge_shift)
            b = jnp.zeros((ch, width), F32) if inner is None else roll(inner, inner_shift)
            return jnp.where(mask, a, b)

        def columns(di):
            mid = get(di, 0)
            left = pick(low_col, get(di, -1), 1 - tc, mid, 1)
            right = pick(high_col, get(di, 1), tc - 1, mid, -1)
            return left, mid, right

        above, here, below = columns(-1), columns(0), columns(1)
        reach = (tr - 1) * tc
        parts = [pick(low_row, a, -reach, h, tc) for a, h in zip(above, here)]
        parts += list(here)
        parts += [pick(high_row, b, reach, h, -tc) for b, h in zip(below, here)]
        patches = jnp.concatenate(parts, axis=0)
        full = finish(patches)
        row3 = lax.broadcasted_iota(jnp.int32, full.shape, 0)
        cell3 = lax.broadcasted_iota(jnp.int32, full.shape, 1)
        full = jnp.where((row3 == chans) & (cell3 >= cells), -1e30, full)
        stack[t] = full.astype(BF)

    def finish(patches):
        twice = jnp.concatenate([patches, patches], axis=0).astype(BF)
        feats = mm(conv_t, twice)
        variance = jnp.sum(feats * feats, axis=0, keepdims=True) * (1.0 / conv_t.shape[0])
        scaled = patches * lax.rsqrt(variance + 1e-05)
        hi, lo = split(scaled)
        full = jnp.concatenate([hi, hi, lo], axis=0)
        row3 = lax.broadcasted_iota(jnp.int32, full.shape, 0)
        return jnp.where(row3 == chans + 1, 1.0, full)

    def attend(block_px, first):
        scores = mm(q3, block_px)
        high = jnp.max(scores, axis=-1, keepdims=True)
        if not first:
            high = jnp.maximum(high, top[...])
        expo = jnp.exp2(scores - high).astype(BF)
        part = mm_nt(expo, block_px)
        if first:
            acc[...] = part
        else:
            acc[...] = acc[...] * jnp.exp2(top[...] - high) + part
        top[...] = high

    def build_frame():
        frame = jnp.concatenate([tiles[t].astype(F32)[:, :cells] for t in range(g)], axis=1)
        span = g * cells
        code = code_ref[...]
        low_c, high_c, low_r, high_r, left_t, right_t, top_t, bottom_t = (
            (code & (1 << bit)) != 0 for bit in range(8)
        )

        def shifted(x, edge, outside, far, near):
            far_x = jnp.where(outside, 0.0, pltpu.roll(x, far % span, 1))
            return jnp.where(edge, far_x, pltpu.roll(x, near % span, 1))

        side = cells - (tc - 1)
        over = ngy * cells - (tr - 1) * tc
        here = (
            shifted(frame, low_c, left_t, side, 1),
            frame,
            shifted(frame, high_c, right_t, -side, -1),
        )
        parts = [shifted(x, low_r, top_t, over, tc) for x in here]
        parts += list(here)
        parts += [shifted(x, high_r, bottom_t, -over, -tc) for x in here]
        for s, part in enumerate(parts):
            patch_ref[s * ch : (s + 1) * ch, :] = part

    if compact:
        build_frame()
        step = 2 * width
        starts = list(range(0, g * cells, step))
        for start in starts:
            stop = min(start + step, g * cells)
            stack[:, start:stop] = finish(patch_ref[:, start:stop]).astype(BF)
        for start in starts:
            stop = min(start + step, g * cells)
            attend(stack[:, start:stop], start == 0)
    else:
        pl.loop(0, g)(build)
        attend(stack[0], True)
        pl.loop(1, g)(lambda t: attend(stack[t], False))

    summed = acc[...]
    lane_s = lax.broadcasted_iota(jnp.int32, summed.shape, 1)
    total = jnp.sum(jnp.where(lane_s == chans + 1, summed, 0.0), axis=-1, keepdims=True)
    mv_hi, mv_lo = split(mv)
    zero = jnp.zeros_like(mv_lo)
    mv3 = jnp.concatenate(
        [
            jnp.concatenate([mv_hi] * 3, axis=0),
            jnp.concatenate([mv_lo, zero, zero], axis=0),
        ],
        axis=1,
    ).astype(BF)
    s_hi, s_lo = split(summed)
    summed3 = jnp.where((lane_s >= pk) & (lane_s < 2 * pk), s_lo, s_hi).astype(BF)
    both = mm(summed3, mv3)
    attended = (both[:, :DH] + both[:, DH:]) / total
    att_src[...] = attended.astype(BF).reshape(heads, share, DH)

    mine = pltpu.make_async_copy(att_src.at[head], att.at[head], copy_sem.at[7])
    mine.start()
    sends2 = []
    for k in range(1, heads):
        to = lax.rem(head + k, heads)
        send = pltpu.make_async_remote_copy(
            src_ref=att_src.at[to],
            dst_ref=att.at[head],
            send_sem=send2.at[k],
            recv_sem=recv2.at[k],
            device_id=place(block * heads + to),
            device_id_type=MESH,
        )
        send.start()
        sends2.append(send)
    for send in sends:
        send.wait_send()
    loads[5].wait()
    loads[6].wait()
    mine.wait()
    for k in range(1, heads):
        source = lax.rem(head + heads - k, heads)
        came = pltpu.make_async_remote_copy(
            src_ref=att_src.at[source],
            dst_ref=att.at[source],
            send_sem=send2.at[k],
            recv_sem=recv2.at[k],
            device_id=place(block * heads + source),
            device_id_type=MESH,
        )
        came.wait_recv()
    gathered = jnp.concatenate([att[h] for h in range(heads)], axis=1)
    out_ref[...] = (own[...].astype(F32) + mm(gathered, wo[...])).astype(BF)
    for send in sends2:
        send.wait_send()


def on_device(
    pixels,
    conv_weight,
    input_gain,
    key_weight,
    value_weight,
    latents,
    latent_gain,
    query_weight,
    out_weight,
):
    tr, tc, chans = pixels.shape
    ngx, ngy = lax.axis_size("gx"), lax.axis_size("gy")
    g = ngx * ngy
    lat_count, width_d = latents.shape
    heads = width_d // DH
    share = lat_count // g
    rows = share * heads
    feat = conv_weight.shape[1]
    taps = conv_weight.shape[0] // chans
    width = -(-tr * tc // 128) * 128
    ch = -(-(chans + 2) // 8) * 8
    planes = jnp.transpose(pixels, (2, 0, 1))
    pk = taps * ch
    compact = g <= 8
    vmem = pl.BlockSpec(memory_space=pltpu.VMEM)
    hbm = pl.BlockSpec(memory_space=pl.ANY)
    return pl.pallas_call(
        functools.partial(kernel, (ngx, ngy, tr, tc, heads, taps, chans)),
        out_shape=jax.ShapeDtypeStruct((share, width_d), BF),
        in_specs=[hbm] * 9,
        out_specs=vmem,
        scratch_shapes=[
            pltpu.VMEM((chans, tr, tc), BF),
            pltpu.VMEM((ch, width), F32),
            pltpu.VMEM((ch, width), BF),
            pltpu.VMEM(conv_weight.shape, BF),
            pltpu.VMEM((feat,), F32),
            pltpu.VMEM((width_d,), F32),
            pltpu.VMEM((ch, g * tr * tc if compact else 128), jnp.int32),
            pltpu.VMEM((pk, g * tr * tc if compact else 128), F32),
            pltpu.VMEM((g, ch, width), BF),
            pltpu.VMEM((3 * pk, g * tr * tc) if compact else (g, 3 * pk, width), BF),
            pltpu.VMEM((pk, feat), F32),
            pltpu.VMEM((feat, DH), BF),
            pltpu.VMEM((feat, DH), BF),
            pltpu.VMEM((width_d, DH), BF),
            pltpu.VMEM((rows, width_d), BF),
            pltpu.VMEM((share, width_d), BF),
            pltpu.VMEM((width_d, width_d), BF),
            pltpu.VMEM((rows, 3 * pk), F32),
            pltpu.VMEM((rows, 1), F32),
            pltpu.VMEM((heads, share, DH), BF),
            pltpu.VMEM((heads, share, DH), BF),
            pltpu.SemaphoreType.DMA((12,)),
            pltpu.SemaphoreType.DMA((g,)),
            pltpu.SemaphoreType.DMA((g,)),
            pltpu.SemaphoreType.DMA((heads,)),
            pltpu.SemaphoreType.DMA((heads,)),
        ],
        compiler_params=pltpu.CompilerParams(
            collective_id=0, has_side_effects=True, vmem_limit_bytes=56 * 1024 * 1024
        ),
    )(
        planes,
        conv_weight,
        input_gain,
        latent_gain,
        key_weight,
        value_weight,
        latents,
        query_weight,
        out_weight,
    )


def solution(mesh):
    return jax.shard_map(
        on_device,
        mesh=mesh,
        in_specs=(P(("ba", "gx"), "gy", None), P(), P(), P(), P(), P(), P(), P(), P()),
        out_specs=P(("ba", "gx", "gy"), None),
        check_vma=False,
    )
```

```python
import functools
import math

import jax
import jax.numpy as jnp
from jax import lax
from jax.experimental import pallas as pl
from jax.experimental.pallas import tpu as pltpu
from jax.sharding import PartitionSpec as P

DH = 128
MESH = pl.DeviceIdType.MESH
BF = jnp.bfloat16
F32 = jnp.float32


def mm(a, b, precision=None):
    return lax.dot_general(
        a, b, (((1,), (0,)), ((), ())), precision=precision, preferred_element_type=F32
    )


def mm_nt(a, b):
    return lax.dot_general(a, b, (((1,), (1,)), ((), ())), preferred_element_type=F32)


def split(x):
    hi = x.astype(BF).astype(F32)
    return hi, x - hi


def kernel(
    dims,
    px_hbm,
    conv_hbm,
    gain_hbm,
    lgain_hbm,
    wk_ref,
    wv_ref,
    lat_ref,
    wq_ref,
    wo_ref,
    out_ref,
    px_raw,
    px_wide,
    px_ref,
    conv_ref,
    gain_ref,
    lgain_ref,
    code_ref,
    patch_ref,
    tiles,
    stack,
    conv8,
    wk,
    wv,
    wq,
    lat,
    own,
    wo,
    acc,
    top,
    q_ref,
    att_src,
    att,
    copy_sem,
    send1,
    recv1,
    send2,
    recv2,
):
    ngx, ngy, tr, tc, heads, taps, chans = dims
    g = ngx * ngy
    blocks = g // heads
    share = own.shape[0]
    rows = lat.shape[0]
    width = px_ref.shape[1]
    compact = g <= 8
    cells = tr * tc
    ch = px_ref.shape[0]
    pk = taps * ch
    me = lax.axis_index("gx") * ngy + lax.axis_index("gy")
    head = lax.rem(me, heads)
    block = me // heads

    col = pl.ds(pl.multiple_of(head * DH, DH), DH)
    lat_rows = pl.ds(pl.multiple_of(block * rows, rows), rows)
    own_rows = pl.ds(pl.multiple_of(me * share, share), share)
    def place(p):
        return {"gx": p // ngy, "gy": lax.rem(p, ngy)}

    barrier = pltpu.get_barrier_semaphore()
    for k in range(1, g):
        pl.semaphore_signal(
            barrier, inc=1, device_id=place(lax.rem(me + k, g)), device_id_type=MESH
        )
    early = [
        pltpu.make_async_copy(px_hbm, px_raw, copy_sem.at[8]),
        pltpu.make_async_copy(conv_hbm, conv_ref, copy_sem.at[9]),
        pltpu.make_async_copy(gain_hbm, gain_ref, copy_sem.at[10]),
        pltpu.make_async_copy(lgain_hbm, lgain_ref, copy_sem.at[11]),
    ]
    for load in early:
        load.start()
    own_tile = pltpu.make_async_copy(px_ref, tiles.at[me], copy_sem.at[0])
    loads = [
        own_tile,
        pltpu.make_async_copy(lat_ref.at[lat_rows, :], lat, copy_sem.at[1]),
        pltpu.make_async_copy(wq_ref.at[:, col], wq, copy_sem.at[2]),
        pltpu.make_async_copy(wk_ref.at[:, col], wk, copy_sem.at[3]),
        pltpu.make_async_copy(wv_ref.at[:, col], wv, copy_sem.at[4]),
        pltpu.make_async_copy(lat_ref.at[own_rows, :], own, copy_sem.at[5]),
        pltpu.make_async_copy(wo_ref, wo, copy_sem.at[6]),
    ]
    for load in loads[1:]:
        load.start()

    px_wide[...] = jnp.zeros_like(px_wide)
    if compact:
        spot = lax.broadcasted_iota(jnp.int32, (ch, g * cells), 1)
        tile = spot // cells
        inner = spot - tile * cells
        r = inner // tc
        c = inner - r * tc
        ti = tile // ngy
        tj = tile - ti * ngy
        code = jnp.zeros_like(spot)
        tests = (
            c == 0, c == tc - 1, r == 0, r == tr - 1,
            tj == 0, tj == ngy - 1, ti == 0, ti == ngx - 1,
        )
        for bit, test in enumerate(tests):
            code = code + jnp.where(test, 1 << bit, 0)
        code_ref[...] = code
    early[0].wait()
    raw = px_raw[...].astype(F32)
    px_wide[0:chans, 0:cells] = jnp.concatenate([raw[:, r, :] for r in range(tr)], axis=1)
    px_ref[...] = px_wide[...].astype(BF)
    own_tile.start()
    pl.semaphore_wait(barrier, g - 1)
    sends = []
    for k in range(1, g):
        send = pltpu.make_async_remote_copy(
            src_ref=px_ref,
            dst_ref=tiles.at[me],
            send_sem=send1.at[k],
            recv_sem=recv1.at[k],
            device_id=place(lax.rem(me + k, g)),
            device_id_type=MESH,
        )
        send.start()
        sends.append(send)

    for load in early[1:]:
        load.wait()
    conv8[...] = jnp.zeros_like(conv8)
    for s in range(taps):
        conv8[s * ch : s * ch + chans, :] = conv_ref[s * chans : (s + 1) * chans, :].astype(F32)
    conv = conv8[...]
    centred = conv - jnp.mean(conv, axis=-1, keepdims=True)
    gained_hi, gained_lo = split(centred * gain_ref[...].reshape(1, -1))
    gained = jnp.concatenate([gained_hi, gained_lo], axis=0).astype(BF)
    doubled = jnp.transpose(jnp.concatenate([centred, centred], axis=0))
    lane2 = lax.broadcasted_iota(jnp.int32, doubled.shape, 1)
    d_hi, d_lo = split(doubled)
    conv_t = jnp.where(lane2 < pk, d_hi, d_lo).astype(BF)

    loads[1].wait()
    loads[2].wait()
    rows_f = lat[...].astype(F32)
    mean = jnp.mean(rows_f, axis=-1, keepdims=True)
    rows_c = rows_f - mean
    var = jnp.mean(rows_c * rows_c, axis=-1, keepdims=True)
    lat_normed = (rows_c * lax.rsqrt(var + 1e-05) * lgain_ref[...].reshape(1, -1)).astype(BF)
    query = mm(lat_normed, wq[...]).astype(BF)
    loads[3].wait()
    loads[4].wait()
    mk2 = mm(gained, wk[...])
    mv2 = mm(gained, wv[...])
    mk = mk2[:pk] + mk2[pk:]
    mv = mv2[:pk] + mv2[pk:]
    mk_hi, mk_lo = split(mk)
    mk3_hi = jnp.concatenate([mk_hi] * 3, axis=0).astype(BF)
    mk3_lo = jnp.concatenate([mk_lo] * 3, axis=0).astype(BF)
    q3 = (mm_nt(query, mk3_hi) + mm_nt(query, mk3_lo)) * (math.log2(math.e) / DH**0.5)
    q_hi, q_lo = split(q3)
    lane3 = lax.broadcasted_iota(jnp.int32, q3.shape, 1)
    q3 = jnp.where((lane3 >= pk) & (lane3 < 2 * pk), q_lo, q_hi)
    q3 = jnp.where(lane3 == chans, 1.0, q3).astype(BF)
    q_ref[...] = q3

    loads[0].wait()
    for k, send in enumerate(sends, 1):
        came = pltpu.make_async_remote_copy(
            src_ref=px_ref,
            dst_ref=tiles.at[lax.rem(me + g - k, g)],
            send_sem=send1.at[k],
            recv_sem=recv1.at[k],
            device_id=place(lax.rem(me + g - k, g)),
            device_id_type=MESH,
        )
        came.wait_recv()

    lane = lax.broadcasted_iota(jnp.int32, (ch, width), 1)
    tile_row = lane // tc
    tile_col = lane - tile_row * tc
    low_row, high_row = tile_row == 0, tile_row == tr - 1
    low_col, high_col = tile_col == 0, tile_col == tc - 1

    def roll(x, shift):
        return pltpu.roll(x, shift % width, 1)

    def build(t):
        static = isinstance(t, int)
        i = t // ngy
        j = t - i * ngy

        def get(di, dj):
            if static:
                if 0 <= i + di < ngx and 0 <= j + dj < ngy:
                    return tiles[t + di * ngy + dj].astype(F32)
                return None
            inside = (i + di >= 0) & (i + di < ngx) & (j + dj >= 0) & (j + dj < ngy)
            at = jnp.clip(t + di * ngy + dj, 0, g - 1)
            return tiles[at].astype(F32) * jnp.where(inside, 1.0, 0.0)

        def pick(mask, edge, edge_shift, inner, inner_shift):
            if inner is None and edge is None:
                return None
            a = jnp.zeros((ch, width), F32) if edge is None else roll(edge, edge_shift)
            b = jnp.zeros((ch, width), F32) if inner is None else roll(inner, inner_shift)
            return jnp.where(mask, a, b)

        def columns(di):
            mid = get(di, 0)
            left = pick(low_col, get(di, -1), 1 - tc, mid, 1)
            right = pick(high_col, get(di, 1), tc - 1, mid, -1)
            return left, mid, right

        above, here, below = columns(-1), columns(0), columns(1)
        reach = (tr - 1) * tc
        parts = [pick(low_row, a, -reach, h, tc) for a, h in zip(above, here)]
        parts += list(here)
        parts += [pick(high_row, b, reach, h, -tc) for b, h in zip(below, here)]
        patches = jnp.concatenate(parts, axis=0)
        full = finish(patches)
        row3 = lax.broadcasted_iota(jnp.int32, full.shape, 0)
        cell3 = lax.broadcasted_iota(jnp.int32, full.shape, 1)
        full = jnp.where((row3 == chans) & (cell3 >= cells), -1e30, full)
        stack[t] = full.astype(BF)

    def finish(patches):
        twice = jnp.concatenate([patches, patches], axis=0).astype(BF)
        feats = mm(conv_t, twice)
        variance = jnp.sum(feats * feats, axis=0, keepdims=True) * (1.0 / conv_t.shape[0])
        scaled = patches * lax.rsqrt(variance + 1e-05)
        hi, lo = split(scaled)
        full = jnp.concatenate([hi, hi, lo], axis=0)
        row3 = lax.broadcasted_iota(jnp.int32, full.shape, 0)
        return jnp.where(row3 == chans + 1, 1.0, full)

    def attend(block_px, first):
        scores = mm(q3, block_px)
        high = jnp.max(scores, axis=-1, keepdims=True)
        if not first:
            high = jnp.maximum(high, top[...])
        expo = jnp.exp2(scores - high).astype(BF)
        part = mm_nt(expo, block_px)
        if first:
            acc[...] = part
        else:
            acc[...] = acc[...] * jnp.exp2(top[...] - high) + part
        top[...] = high

    def build_frame():
        frame = jnp.concatenate([tiles[t].astype(F32)[:, :cells] for t in range(g)], axis=1)
        span = g * cells
        code = code_ref[...]
        low_c, high_c, low_r, high_r, left_t, right_t, top_t, bottom_t = (
            (code & (1 << bit)) != 0 for bit in range(8)
        )

        def shifted(x, edge, outside, far, near):
            far_x = jnp.where(outside, 0.0, pltpu.roll(x, far % span, 1))
            return jnp.where(edge, far_x, pltpu.roll(x, near % span, 1))

        side = cells - (tc - 1)
        over = ngy * cells - (tr - 1) * tc
        here = (
            shifted(frame, low_c, left_t, side, 1),
            frame,
            shifted(frame, high_c, right_t, -side, -1),
        )
        parts = [shifted(x, low_r, top_t, over, tc) for x in here]
        parts += list(here)
        parts += [shifted(x, high_r, bottom_t, -over, -tc) for x in here]
        for s, part in enumerate(parts):
            patch_ref[s * ch : (s + 1) * ch, :] = part

    if compact:
        build_frame()
        step = 2 * width
        starts = list(range(0, g * cells, step))
        for start in starts:
            stop = min(start + step, g * cells)
            stack[:, start:stop] = finish(patch_ref[:, start:stop]).astype(BF)
    else:
        pl.loop(0, g)(build)
        attend(stack[0], True)
        pl.loop(1, g)(lambda t: attend(stack[t], False))

    def finalize(summed):
        lane_s = lax.broadcasted_iota(jnp.int32, summed.shape, 1)
        total = jnp.sum(jnp.where(lane_s == chans + 1, summed, 0.0), axis=-1, keepdims=True)
        mv_hi, mv_lo = split(mv)
        zero = jnp.zeros_like(mv_lo)
        mv3 = jnp.concatenate(
            [
                jnp.concatenate([mv_hi] * 3, axis=0),
                jnp.concatenate([mv_lo, zero, zero], axis=0),
            ],
            axis=1,
        ).astype(BF)
        s_hi, s_lo = split(summed)
        summed3 = jnp.where((lane_s >= pk) & (lane_s < 2 * pk), s_lo, s_hi).astype(BF)
        both = mm(summed3, mv3)
        attended = (both[:, :DH] + both[:, DH:]) / total
        return attended.astype(BF)

    half = heads // 2
    far = 1 - head // half
    spot_h = lax.rem(head, half)
    sends2 = []
    routes = []

    def exchange(part, count_from, slot):
        for m in range(count_from, half):
            to = part * half + lax.rem(spot_h + m, half)
            source = part * half + lax.rem(spot_h + half - m, half)
            send = pltpu.make_async_remote_copy(
                src_ref=att_src.at[to],
                dst_ref=att.at[head],
                send_sem=send2.at[slot + m],
                recv_sem=recv2.at[slot + m],
                device_id=place(block * heads + to),
                device_id_type=MESH,
            )
            send.start()
            sends2.append(send)
            routes.append((source, slot + m))

    if compact:
        piece = rows // 2
        for part in (far, 1 - far):
            query_part = q_ref[pl.ds(pl.multiple_of(part * piece, piece), piece), :]
            summed, peak = None, None
            for start in starts:
                block_px = stack[:, start : min(start + step, g * cells)]
                scores = mm(query_part, block_px)
                high = jnp.max(scores, axis=-1, keepdims=True)
                if summed is not None:
                    high = jnp.maximum(high, peak)
                expo = jnp.exp2(scores - high).astype(BF)
                added = mm_nt(expo, block_px)
                summed = added if summed is None else summed * jnp.exp2(peak - high) + added
                peak = high
            att_src[pl.ds(part * half, half)] = finalize(summed).reshape(half, share, DH)
            if part is far:
                exchange(far, 0, 0)
        mine = pltpu.make_async_copy(att_src.at[head], att.at[head], copy_sem.at[7])
        mine.start()
        exchange(1 - far, 1, half)
    else:
        att_src[...] = finalize(acc[...]).reshape(heads, share, DH)
        exchange(far, 0, 0)
        mine = pltpu.make_async_copy(att_src.at[head], att.at[head], copy_sem.at[7])
        mine.start()
        exchange(1 - far, 1, half)
    for send in sends:
        send.wait_send()
    loads[5].wait()
    loads[6].wait()
    mine.wait()
    for source, slot in routes:
        came = pltpu.make_async_remote_copy(
            src_ref=att_src.at[source],
            dst_ref=att.at[source],
            send_sem=send2.at[slot],
            recv_sem=recv2.at[slot],
            device_id=place(block * heads + source),
            device_id_type=MESH,
        )
        came.wait_recv()
    gathered = jnp.concatenate([att[h] for h in range(heads)], axis=1)
    out_ref[...] = (own[...].astype(F32) + mm(gathered, wo[...])).astype(BF)
    for send in sends2:
        send.wait_send()


def on_device(
    pixels,
    conv_weight,
    input_gain,
    key_weight,
    value_weight,
    latents,
    latent_gain,
    query_weight,
    out_weight,
):
    tr, tc, chans = pixels.shape
    ngx, ngy = lax.axis_size("gx"), lax.axis_size("gy")
    g = ngx * ngy
    lat_count, width_d = latents.shape
    heads = width_d // DH
    share = lat_count // g
    rows = share * heads
    feat = conv_weight.shape[1]
    taps = conv_weight.shape[0] // chans
    width = -(-tr * tc // 128) * 128
    ch = -(-(chans + 2) // 8) * 8
    planes = jnp.transpose(pixels, (2, 0, 1))
    pk = taps * ch
    compact = g <= 8
    vmem = pl.BlockSpec(memory_space=pltpu.VMEM)
    hbm = pl.BlockSpec(memory_space=pl.ANY)
    return pl.pallas_call(
        functools.partial(kernel, (ngx, ngy, tr, tc, heads, taps, chans)),
        out_shape=jax.ShapeDtypeStruct((share, width_d), BF),
        in_specs=[hbm] * 9,
        out_specs=vmem,
        scratch_shapes=[
            pltpu.VMEM((chans, tr, tc), BF),
            pltpu.VMEM((ch, width), F32),
            pltpu.VMEM((ch, width), BF),
            pltpu.VMEM(conv_weight.shape, BF),
            pltpu.VMEM((feat,), F32),
            pltpu.VMEM((width_d,), F32),
            pltpu.VMEM((ch, g * tr * tc if compact else 128), jnp.int32),
            pltpu.VMEM((pk, g * tr * tc if compact else 128), F32),
            pltpu.VMEM((g, ch, width), BF),
            pltpu.VMEM((3 * pk, g * tr * tc) if compact else (g, 3 * pk, width), BF),
            pltpu.VMEM((pk, feat), F32),
            pltpu.VMEM((feat, DH), BF),
            pltpu.VMEM((feat, DH), BF),
            pltpu.VMEM((width_d, DH), BF),
            pltpu.VMEM((rows, width_d), BF),
            pltpu.VMEM((share, width_d), BF),
            pltpu.VMEM((width_d, width_d), BF),
            pltpu.VMEM((rows, 3 * pk), F32),
            pltpu.VMEM((rows, 1), F32),
            pltpu.VMEM((rows, 3 * pk), BF),
            pltpu.VMEM((heads, share, DH), BF),
            pltpu.VMEM((heads, share, DH), BF),
            pltpu.SemaphoreType.DMA((12,)),
            pltpu.SemaphoreType.DMA((g,)),
            pltpu.SemaphoreType.DMA((g,)),
            pltpu.SemaphoreType.DMA((heads,)),
            pltpu.SemaphoreType.DMA((heads,)),
        ],
        compiler_params=pltpu.CompilerParams(
            collective_id=0, has_side_effects=True, vmem_limit_bytes=56 * 1024 * 1024
        ),
    )(
        planes,
        conv_weight,
        input_gain,
        latent_gain,
        key_weight,
        value_weight,
        latents,
        query_weight,
        out_weight,
    )


def solution(mesh):
    return jax.shard_map(
        on_device,
        mesh=mesh,
        in_specs=(P(("ba", "gx"), "gy", None), P(), P(), P(), P(), P(), P(), P(), P()),
        out_specs=P(("ba", "gx", "gy"), None),
        check_vma=False,
    )
```
